512 devices in a mesh: lon: 32 (over y_hi, z, core), lat: 16 (over y_lo, x).
Axes of the slice: x: 4, y: 8 (y_hi: 2, y_lo: 4; y = y_hi * 4 + y_lo), z: 8, core: 2. Of those that a mesh axis runs over, the one named last changes fastest.
Arguments:
- fine_input: bfloat16 [4, 192, 768, 384], P(None, 'lat', 'lon'), may hold values from -10 to 10
- merge_gain: float32 [1536], replicated, may hold values from 0.5 to 1.5
- merge_bias: float32 [1536], replicated, may hold values from -1.5 to 1.5
- merge_weight: bfloat16 [1536, 768], P('lat'), may hold values from -2 to 2
- coarse_gain: float32 [768], replicated, may hold values from 0.5 to 1.5
- coarse_bias: float32 [768], replicated, may hold values from -1.5 to 1.5
- coarse_qkv: bfloat16 [768, 2304], P('lat'), may hold values from -2 to 2
- coarse_out: bfloat16 [768, 768], P('lat'), may hold values from -0.21875 to 0.21875
Outputs:
- coarse_output: bfloat16 [4, 96, 384, 768], P(None, 'lat', 'lon')
The draws below stay inside these ranges and needn't reach their ends.
All inputs are finite; a program needn't handle non-finite values.
Results may differ from the reference program's by a relative error of at most 0.013.
Values may be sent and summed in bfloat16 or wider, within the bound.
No kernel may reach another device: no remote copies, remote signals or barrier semaphores. Data moves between devices by JAX's collectives and lax.ppermute only.
A program may use at most 128 MiB of HBM per device.

```python
import jax
import jax.numpy as jnp
from jax import lax

WIDTH = 384
WIDTH2 = 768
HEADS2 = 24
LEVELS = 4
LAT = 192
LON = 768


def draw_fine_input(key, part):
    noise_key = jax.random.fold_in(key, 11)
    values = jax.random.truncated_normal(noise_key, -6.0, 6.0, (LEVELS, LAT, LON, WIDTH))
    return values.astype(jnp.bfloat16)


def draw_merge_weight(key, part):
    values = jax.random.truncated_normal(jax.random.fold_in(key, 14), -4.0, 4.0, (4 * WIDTH, WIDTH2)) / jnp.sqrt(4.0 * WIDTH)
    return values.astype(jnp.bfloat16)


def draw_coarse_qkv(key, part):
    values = jax.random.truncated_normal(jax.random.fold_in(key, 15), -4.0, 4.0, (WIDTH2, 3 * WIDTH2)) / jnp.sqrt(1.0 * WIDTH2)
    return values.astype(jnp.bfloat16)


def block_levels(rng, extent, shards, least, largest):
    loudness, own = 1.0, jax.random.fold_in(rng, 6)
    for axis_at, shards_of in shards:
        heights = jnp.exp(jax.random.uniform(jax.random.fold_in(own, axis_at), (shards_of,), jnp.float32, least / len(shards), largest / len(shards)))
        loudness = loudness * jnp.repeat(heights, extent[axis_at] // shards_of).reshape([-1 if axis == axis_at else 1 for axis in range(len(extent))])
    return loudness


def scatter_about(key, extent, deviation, most, split=(), kind=jnp.bfloat16):
    loudness = block_levels(key, extent, split, -0.22, 0.18) if split else 1.0
    entries = jax.random.normal(key, extent, jnp.float32) * deviation * loudness
    return jnp.minimum(jnp.maximum(entries, -most), most).astype(kind)


def setup_inputs(seed: int = 0) -> dict:
    key_of = jax.random.split(jax.random.key(seed), 9)
    fine_input = draw_fine_input(jax.random.fold_in(key_of[8], 71), 0)
    merge_gain = jnp.clip(1.0 + 0.1 * jax.random.normal(key_of[1], (4 * WIDTH,), jnp.float32), 0.5, 1.5)
    merge_bias = scatter_about(key_of[2], (4 * WIDTH,), 0.3, 1.5, (), jnp.float32)
    merge_weight = draw_merge_weight(jax.random.fold_in(key_of[8], 71), 0)
    coarse_gain = jnp.clip(1.0 + 0.1 * jax.random.normal(key_of[4], (WIDTH2,), jnp.float32), 0.5, 1.5)
    coarse_bias = scatter_about(key_of[5], (WIDTH2,), 0.3, 1.5, (), jnp.float32)
    coarse_qkv = draw_coarse_qkv(jax.random.fold_in(key_of[8], 71), 0)
    coarse_out = scatter_about(key_of[7], (WIDTH2, WIDTH2), WIDTH2 ** -0.5, 0.21875, ((0, 16),))
    return dict(fine_input=fine_input, merge_gain=merge_gain, merge_bias=merge_bias, merge_weight=merge_weight, coarse_gain=coarse_gain, coarse_bias=coarse_bias, coarse_qkv=coarse_qkv, coarse_out=coarse_out)


EPSILON = 1e-05

def normalize(values, norm_gain, norm_bias):
    average = lax.optimization_barrier(jnp.mean(values, axis=-1, keepdims=True))
    centered = values - average
    spread = lax.optimization_barrier(jnp.mean(centered * centered, axis=-1, keepdims=True))
    return centered * lax.rsqrt(spread + EPSILON) * norm_gain + norm_bias

def group_ids(level_count, row_start, row_count, row_total):
    level_index = (jnp.arange(level_count, dtype=jnp.int32) + 1) % level_count
    row_index = (row_start + jnp.arange(row_count, dtype=jnp.int32) + 3) % row_total
    level_group = jnp.floor_divide(level_index - 1, 2)
    row_group = jnp.floor_divide(row_index - 3, 6)
    return level_group[:, None] * 65536 + row_group[None, :]

def attend(framed, group_grid, qkv_weight, head_count):
    level_count, row_count, col_count, width = framed.shape
    head_depth = width // head_count
    flat_rows = framed.reshape(-1, width)
    projected = jnp.dot(flat_rows, qkv_weight, preferred_element_type=jnp.float32).astype(jnp.bfloat16)
    window_shape = (level_count // 2, 2, row_count // 6, 6, col_count // 12, 12)
    windows = projected.reshape(window_shape + (3, head_count, head_depth))
    windows = windows.transpose(0, 2, 4, 1, 3, 5, 6, 7, 8).reshape(-1, 144, 3, head_count, head_depth)
    key_grid = jnp.broadcast_to(group_grid[:, :, None], (level_count, row_count, col_count))
    key_windows = key_grid.reshape(window_shape).transpose(0, 2, 4, 1, 3, 5).reshape(-1, 144)
    allowed = key_windows[:, :, None] == key_windows[:, None, :]
    queries = windows[:, :, 0].astype(jnp.float32)
    keys_all = windows[:, :, 1].astype(jnp.float32)
    values = windows[:, :, 2].astype(jnp.float32)
    scores = jnp.einsum('wqhd,wkhd->whqk', queries, keys_all) * head_depth ** (-0.5)
    scores = jnp.where(allowed[:, None], scores, -jnp.inf)
    row_peak = lax.optimization_barrier(jnp.max(scores, axis=-1, keepdims=True))
    weights = jnp.exp(scores - row_peak)
    probabilities = (weights / lax.optimization_barrier(jnp.sum(weights, axis=-1, keepdims=True))).astype(jnp.bfloat16)
    context = jnp.einsum('whqk,wkhd->wqhd', probabilities.astype(jnp.float32), values).astype(jnp.bfloat16)
    context = context.reshape(level_count // 2, row_count // 6, col_count // 12, 2, 6, 12, width)
    return context.transpose(0, 3, 1, 4, 2, 5, 6).reshape(level_count, row_count, col_count, width)

def sublayer(inputs, norm_gain, norm_bias, qkv_weight, out_weight, head_count):
    level_count, row_total, col_total, width = inputs.shape
    blocks = row_total // 6
    normed = normalize(inputs.astype(jnp.float32), norm_gain, norm_bias).astype(jnp.bfloat16)
    framed = jnp.roll(normed, (-1, -3, -6), axis=(0, 1, 2))
    slabs = framed.reshape(level_count, blocks, 6, col_total, width).transpose(1, 0, 2, 3, 4)

    def one_slab(pair_items):
        slab_rows, block_index = pair_items
        grid_ids = group_ids(level_count, block_index * 6, 6, row_total)
        return attend(slab_rows, grid_ids, qkv_weight, head_count)
    context = lax.map(one_slab, (slabs, jnp.arange(blocks, dtype=jnp.int32)))
    context = context.transpose(1, 0, 2, 3, 4).reshape(level_count, row_total, col_total, width)
    context = jnp.roll(context, (1, 3, 6), axis=(0, 1, 2))
    in_blocks = inputs.reshape(level_count, blocks, 6, col_total, width).transpose(1, 0, 2, 3, 4)
    context_blocks = context.reshape(level_count, blocks, 6, col_total, width).transpose(1, 0, 2, 3, 4)

    def finish(pair_items):
        part_in, part_context = pair_items
        branch = jnp.dot(part_context.reshape(-1, width), out_weight, preferred_element_type=jnp.float32)
        return (part_in.astype(jnp.float32) + branch.reshape(part_in.shape)).astype(jnp.bfloat16)
    result = lax.map(finish, (in_blocks, context_blocks))
    return result.transpose(1, 0, 2, 3, 4).reshape(inputs.shape)

def merge_patches(fine, norm_gain, norm_bias, weight):
    level_count, row_total, col_total, width = fine.shape
    patches = fine.reshape(level_count, row_total // 2, 2, col_total // 2, 2, width)
    patches = patches.transpose(0, 1, 3, 2, 4, 5).reshape(level_count, row_total // 2, col_total // 2, 4 * width)
    normed = normalize(patches.astype(jnp.float32), norm_gain, norm_bias).astype(jnp.bfloat16)
    merged = jnp.dot(normed.reshape(-1, 4 * width), weight, preferred_element_type=jnp.float32)
    return merged.astype(jnp.bfloat16).reshape(level_count, row_total // 2, col_total // 2, weight.shape[1])

def reference(fine_input, merge_gain, merge_bias, merge_weight, coarse_gain, coarse_bias, coarse_qkv, coarse_out):
    coarse_input = merge_patches(fine_input, merge_gain, merge_bias, merge_weight)
    return sublayer(coarse_input, coarse_gain, coarse_bias, coarse_qkv, coarse_out, HEADS2)
```

```python
import jax
import jax.numpy as jnp
from jax import lax
from jax.experimental import pallas as pl
from jax.experimental.pallas import tpu as pltpu
from jax.sharding import PartitionSpec as P


EPSILON = 1e-05
AXES = ("lon", "lat")
F32 = jnp.float32
BF16 = jnp.bfloat16

DEVICES = 512


def coords_of(flat):
    lat, lon = flat % 16, flat // 16
    return lat % 4, (lon // 16) * 4 + lat // 4, lon // 2 % 8, lon % 2


def flat_of(x, y, z, core):
    x, y, z = x % 4, y % 8, z % 8
    return (((y // 4) * 8 + z) * 2 + core) * 16 + (y % 4) * 4 + x


def ring_step(dx, dy, x, y):
    if dy == 2:
        dy = 2 if y % 2 == 0 else -2
    return x + dx, y + dy


def far_pairs(step):
    pairs = []
    for flat in range(DEVICES):
        x, y, z, core = coords_of(flat)
        nx, ny = ring_step(step if core == 1 else 0, step if core == 0 else 0, x, y)
        pairs.append((flat, flat_of(nx, ny, z, core)))
    return pairs


def near_groups():
    groups = {}
    for flat in range(DEVICES):
        x, y, z, core = coords_of(flat)
        key = (core, y, z) if core == 0 else (core, x, z, y // 4)
        groups.setdefault(key, []).append((x if core == 0 else y, flat))
    return [[flat for _, flat in sorted(group)] for group in groups.values()]


def swap_pairs():
    pairs = []
    for flat in range(DEVICES):
        x, y, z, core = coords_of(flat)
        pairs.append((flat, flat_of(x, y, z, 1 - core)))
    return pairs


def shift_pairs(dlon, dlat, back=False):
    pairs = []
    for flat in range(DEVICES):
        lon, lat = flat // 16, flat % 16
        sign = 1 if lon % 2 == 0 else -1
        target = (lon + dlon) % 32 * 16 + (lat + sign * dlat) % 16
        pairs.append((target, flat) if back else (flat, target))
    return pairs


def moved(value, pairs):
    return lax.ppermute(value, AXES, pairs)


STEPS = (0, -1, 1, 2)


def dot(a, b):
    return jnp.dot(a, b, preferred_element_type=F32)


def normalize(values, gain, bias):
    average = jnp.mean(values, axis=-1, keepdims=True)
    centered = values - average
    spread = jnp.mean(centered * centered, axis=-1, keepdims=True)
    return centered * lax.rsqrt(spread + EPSILON) * gain + bias


def cut_kernel(fine_ref, merge_hbm, qkv_hbm, out_hbm, left_ref, held_hbm, sems):
    core = lax.axis_index("lon") % 2
    for side in range(2):

        @pl.when(core == side)
        def _():
            cuts = [(merge_hbm, side * 384, 0, 96), (out_hbm, side * 384, 240, 48)]
            cuts += [(qkv_hbm, side * 1152 + n * 384, 96 + n * 48, 48) for n in range(3)]
            copies = []
            for member in range(4):
                for n, (source, column, row, rows) in enumerate(cuts):
                    copies.append(
                        pltpu.make_async_copy(
                            source.at[:, pl.ds(column, 384)],
                            held_hbm.at[member, pl.ds(row, rows), :],
                            sems.at[member * 5 + n],
                        )
                    )
            for copy in copies:
                copy.start()
            row = lax.broadcasted_iota(jnp.int32, (144, 1), 0)
            source = lax.broadcasted_iota(jnp.int32, (144, 288), 1)
            pick = jnp.where(source == row // 12 * 24 + row % 12, 1.0, 0.0).astype(BF16)
            for level in range(4):
                part = dot(pick, fine_ref[level * 288 : level * 288 + 288])
                left_ref[level * 144 : level * 144 + 144] = part.astype(BF16)
            for copy in copies:
                copy.wait()


def cut(fine, weights):
    vmem = pl.BlockSpec(memory_space=pltpu.VMEM)
    return pl.pallas_call(
        cut_kernel,
        out_shape=(
            jax.ShapeDtypeStruct((576, 384), BF16),
            jax.ShapeDtypeStruct((4, 288, 384), BF16),
        ),
        in_specs=[vmem] * 4,
        out_specs=(vmem, vmem),
        scratch_shapes=[pltpu.SemaphoreType.DMA((20,))],
        name="cut",
        cost_estimate=pl.CostEstimate(flops=1_000_000, bytes_accessed=1_800_000, transcendentals=0),
    )(fine, *weights)


def patch_kernel(
    fine_hbm, left_hbm, gain_hbm, bias_hbm, near_ref, far_ref, fine_ref, left_ref, gain_ref, bias_ref, sems
):
    core = lax.axis_index("lon") % 2
    loads = [
        pltpu.make_async_copy(source, target, sems.at[n])
        for n, (source, target) in enumerate(
            ((fine_hbm, fine_ref), (left_hbm, left_ref), (gain_hbm, gain_ref), (bias_hbm, bias_ref))
        )
    ]
    for load in loads:
        load.start()
    row = lax.broadcasted_iota(jnp.int32, (72, 1), 0)
    level, a, b = row // 18, row % 18 // 6, row % 6
    own_at = level * 144 + a * 48 + (6 + b) * 2
    next_at = level * 144 + a * 24 + b * 2
    source = lax.broadcasted_iota(jnp.int32, (72, 576), 1)

    def picks(base, places):
        return [jnp.where(source == base + at, 1.0, 0.0).astype(BF16) for at in places]

    own_picks = picks(own_at, (0, 1, 24, 25))
    for load in loads:
        load.wait()
    for half, ref in ((1 - core, near_ref), (core, far_ref)):
        own = jnp.concatenate(
            [
                fine_ref[pl.ds(pl.multiple_of(level * 288 + half * 144, 144), 144), :]
                for level in range(4)
            ],
            axis=0,
        )
        next_picks = picks(next_at + half * 72, (0, 1, 12, 13))
        for first, fine, chosen in ((0, own, own_picks), (72, left_ref[...], next_picks)):
            parts = [dot(pick, fine) for pick in chosen]
            total = parts[0] + parts[1] + parts[2] + parts[3]
            average = jnp.sum(total, axis=-1, keepdims=True) / 1536
            parts = [part - average for part in parts]
            squares = sum(part * part for part in parts)
            scale = lax.rsqrt(jnp.sum(squares, axis=-1, keepdims=True) / 1536 + EPSILON)
            for k in range(4):
                cols = slice(k * 384, (k + 1) * 384)
                gain, bias = gain_ref[cols].reshape(1, 384), bias_ref[cols].reshape(1, 384)
                ref[first : first + 72, cols] = (parts[k] * scale * gain + bias).astype(BF16)


def patches(fine, left, gain, bias):
    pack = jax.ShapeDtypeStruct((144, 1536), BF16)
    operands = (fine, left, gain, bias)
    return pl.pallas_call(
        patch_kernel,
        out_shape=(pack, pack),
        in_specs=[pl.BlockSpec(memory_space=pltpu.HBM)] * 4,
        out_specs=(pl.BlockSpec(memory_space=pltpu.VMEM),) * 2,
        scratch_shapes=[pltpu.VMEM(value.shape, value.dtype) for value in operands]
        + [pltpu.SemaphoreType.DMA((4,))],
        name="patches",
        cost_estimate=pl.CostEstimate(
            flops=1_000_000_000, bytes_accessed=1_800_000, transcendentals=0
        ),
    )(*operands)


def frame_order(incoming):
    window = lax.broadcasted_iota(jnp.int32, (288, 1) if incoming else (1, 288), 0 if incoming else 1)
    source = lax.broadcasted_iota(jnp.int32, (288, 288), 1 if incoming else 0)
    pair, rest = window // 144, window % 144
    quad, rest = rest // 36, rest % 36
    level = (2 * pair + rest // 18 + 1) % 4
    place = level * 18 + rest % 18 if incoming else rest % 18 * 4 + level
    return jnp.where(source == quad * 72 + place, 1.0, 0.0).astype(BF16)


def main_kernel(
    p0, p1, a0, a1, a2, a3, b0, b1, b2, b3, gain_ref, bias_ref,
    o0, o1, o2, o3,
    patch_s, merge_s, qkv_s, out_s, proj_s, ctx_s, sems,
):
    core, lat = lax.axis_index("lon") % 2, lax.axis_index("lat")
    x, y = lat % 4, lat // 4
    for source, at in ((p0, 0), (p1, 144)):
        target = patch_s.at[pl.ds(at, 144), :]
        pltpu.make_async_copy(source, target, sems.at[0]).start()

    def scatter(kind, source, k, side):
        def part(base, rows, target, sem, first, width):
            spot = (y + STEPS[k] + 4) % 4 if side == 0 else (x + STEPS[k] + 4) % 4
            cols = pl.ds(side * width + first, 384)
            held = source.at[:, pl.ds(base, rows), :]
            place = target.at[spot, :, :, cols] if side == 0 else target.at[:, spot, :, cols]
            pltpu.make_async_copy(held, place, sems.at[sem]).start()

        if kind == 0:
            part(0, 96, merge_s, 1, 0, 384)
        elif kind == 1:
            for n in range(3):
                part(96 + n * 48, 48, qkv_s, 2, n * 384, 1152)
        else:
            part(240, 48, out_s, 3, 0, 384)

    own, other = (a0, a1, a2, a3), (b0, b1, b2, b3)
    for near_core in range(2):

        @pl.when(core == near_core)
        def _():
            for kind in range(3):
                for blocks, side in ((own, near_core), (other, 1 - near_core)):
                    for k in range(4):
                        scatter(kind, blocks[k], k, side)

    to_window = frame_order(True)
    pltpu.make_async_copy(patch_s, patch_s, sems.at[0]).wait()
    pltpu.make_async_copy(merge_s, merge_s, sems.at[1]).wait()
    coarse = dot(patch_s[...], merge_s[...].reshape(1536, 768)).astype(BF16)
    coarse = dot(to_window, coarse).astype(BF16)
    gain, bias = gain_ref[...].reshape(1, 768), bias_ref[...].reshape(1, 768)
    normed = normalize(coarse.astype(F32), gain, bias).astype(BF16)
    pltpu.make_async_copy(qkv_s, qkv_s, sems.at[2]).wait()
    for n in range(6):
        cols = slice(n * 384, (n + 1) * 384)
        proj_s[:, cols] = dot(normed, qkv_s[:, :, :, cols].reshape(768, 384)).astype(BF16)

    lane = lax.broadcasted_iota(jnp.int32, (1, 128), 1) // 32
    query = lax.broadcasted_iota(jnp.int32, (576, 1), 0) % 144
    key = lax.broadcasted_iota(jnp.int32, (1, 144), 1)
    wraps = lat == jnp.where(core == 0, 15, 0)
    row_apart = ((query // 72) != (key // 72)) & wraps
    level_apart = (query // 18 % 2) != (key // 18 % 2)
    low = F32(-1e30)
    for pair in range(2):
        rows = slice(pair * 144, (pair + 1) * 144)
        apart = (row_apart | level_apart) if pair == 1 else row_apart
        penalty = jnp.where(apart, low, 0.0)
        for g in range(6):
            q = proj_s[rows, g * 128 : (g + 1) * 128]
            k = proj_s[rows, 768 + g * 128 : 768 + (g + 1) * 128]
            v = proj_s[rows, 1536 + g * 128 : 1536 + (g + 1) * 128]
            stacked = jnp.concatenate(
                [jnp.where(lane == h, q, jnp.zeros_like(q)) for h in range(4)], axis=0
            )
            scores = lax.dot_general(
                stacked, k, (((1,), (1,)), ((), ())), preferred_element_type=F32
            )
            scores = scores * (32**-0.5) + penalty
            peak = jnp.max(scores, axis=-1, keepdims=True)
            weights = jnp.exp(scores - peak)
            total = jnp.sum(weights, axis=-1, keepdims=True)
            mixed = dot(weights.astype(BF16), v) / total
            picked = mixed[:144] * jnp.where(lane == 0, 1.0, 0.0)
            for h in range(1, 4):
                picked = jnp.where(lane == h, mixed[h * 144 : (h + 1) * 144], picked)
            ctx_s[rows, g * 128 : (g + 1) * 128] = picked.astype(BF16)

    pltpu.make_async_copy(out_s, out_s, sems.at[3]).wait()
    branch = dot(ctx_s[...], out_s[...].reshape(768, 768))
    result = (coarse.astype(F32) + branch).astype(BF16)
    result = dot(frame_order(False), result).astype(BF16)
    for ref, first, count in ((o0, 0, 18), (o1, 72, 18), (o2, 144, 18), (o3, 216, 18)):
        for place in range(count):
            at = first + place * 4
            ref[place] = result[at : at + 4]


def main(quads, own, other, gain, bias):
    any_space = pl.BlockSpec(memory_space=pl.ANY)
    vmem = pl.BlockSpec(memory_space=pltpu.VMEM)
    quad = jax.ShapeDtypeStruct((18, 4, 768), BF16)
    return pl.pallas_call(
        main_kernel,
        out_shape=(quad,) * 4,
        in_specs=[any_space] * 10 + [vmem] * 2,
        out_specs=(vmem,) * 4,
        scratch_shapes=[
            pltpu.VMEM((288, 1536), BF16),
            pltpu.VMEM((4, 4, 96, 768), BF16),
            pltpu.VMEM((4, 4, 48, 2304), BF16),
            pltpu.VMEM((4, 4, 48, 768), BF16),
            pltpu.VMEM((288, 2304), BF16),
            pltpu.VMEM((288, 768), BF16),
            pltpu.SemaphoreType.DMA((4,)),
        ],
        name="main",
        compiler_params=pltpu.CompilerParams(vmem_limit_bytes=32 * 1024 * 1024),
        cost_estimate=pl.CostEstimate(
            flops=5_000_000_000, bytes_accessed=9_000_000, transcendentals=2_000_000
        ),
    )(*quads, *own, *other, gain, bias)


def tiles(quad):
    return quad.reshape(3, 6, 4, 768)


def shards(
    fine_input,
    merge_gain,
    merge_bias,
    merge_weight,
    coarse_gain,
    coarse_bias,
    coarse_qkv,
    coarse_out,
):
    weights = (merge_weight, coarse_qkv, coarse_out)
    fine = fine_input.reshape(1152, 384)
    left, held = cut(fine, weights)
    block = lax.all_to_all(held, AXES, 0, 0, axis_index_groups=near_groups())
    left = moved(left, shift_pairs(-1, 0))
    own = [block] + [moved(block, far_pairs(step)) for step in (1, -1, 2)]
    near_rows, far_rows = patches(fine, left, merge_gain, merge_bias)
    far_rows = moved(far_rows, shift_pairs(0, -1))
    other = []
    for piece in own:
        other.append(moved(piece, swap_pairs()))
    result = main([near_rows, far_rows], own, other, coarse_gain, coarse_bias)
    near_left = moved(result[3], shift_pairs(-1, 1, back=True))
    far_right = moved(result[2], shift_pairs(0, -1, back=True))
    far_left = moved(result[1], shift_pairs(-1, 0, back=True))
    near = [tiles(near_left), tiles(result[0])]
    far = [tiles(far_left), tiles(far_right)]
    upper = lax.axis_index("lon") % 2 == 1
    above = jnp.concatenate([jnp.where(upper, a, b) for a, b in zip(near, far)], axis=1)
    below = jnp.concatenate([jnp.where(upper, b, a) for a, b in zip(near, far)], axis=1)
    return jnp.concatenate([above, below], axis=0).transpose(2, 0, 1, 3)


def solution(mesh):
    placed = (
        P(None, "lat", "lon", None),
        P(),
        P(),
        P("lat", None),
        P(),
        P(),
        P("lat", None),
        P("lat", None),
    )
    return jax.shard_map(
        shards, mesh=mesh, in_specs=placed, out_specs=P(None, "lat", "lon", None), check_vma=False
    )
```

```python
import jax
import jax.numpy as jnp
from jax import lax
from jax.experimental import pallas as pl
from jax.experimental.pallas import tpu as pltpu
from jax.sharding import PartitionSpec as P


EPSILON = 1e-05
AXES = ("lon", "lat")
F32 = jnp.float32
BF16 = jnp.bfloat16

DEVICES = 512


def coords_of(flat):
    lat, lon = flat % 16, flat // 16
    return lat % 4, (lon // 16) * 4 + lat // 4, lon // 2 % 8, lon % 2


def flat_of(x, y, z, core):
    x, y, z = x % 4, y % 8, z % 8
    return (((y // 4) * 8 + z) * 2 + core) * 16 + (y % 4) * 4 + x


def ring_step(dx, dy, x, y):
    if dy == 2:
        dy = 2 if y % 2 == 0 else -2
    return x + dx, y + dy


def far_pairs(step):
    pairs = []
    for flat in range(DEVICES):
        x, y, z, core = coords_of(flat)
        nx, ny = ring_step(step if core == 1 else 0, step if core == 0 else 0, x, y)
        pairs.append((flat, flat_of(nx, ny, z, core)))
    return pairs


def near_groups():
    groups = {}
    for flat in range(DEVICES):
        x, y, z, core = coords_of(flat)
        key = (core, y, z) if core == 0 else (core, x, z, y // 4)
        groups.setdefault(key, []).append((x if core == 0 else y, flat))
    return [[flat for _, flat in sorted(group)] for group in groups.values()]


def swap_pairs():
    pairs = []
    for flat in range(DEVICES):
        x, y, z, core = coords_of(flat)
        pairs.append((flat, flat_of(x, y, z, 1 - core)))
    return pairs


def shift_pairs(dlon, dlat, back=False):
    pairs = []
    for flat in range(DEVICES):
        lon, lat = flat // 16, flat % 16
        sign = 1 if lon % 2 == 0 else -1
        target = (lon + dlon) % 32 * 16 + (lat + sign * dlat) % 16
        pairs.append((target, flat) if back else (flat, target))
    return pairs


def moved(value, pairs):
    return lax.ppermute(value, AXES, pairs)


STEPS = (0, -1, 1, 2)


def dot(a, b):
    return jnp.dot(a, b, preferred_element_type=F32)


def normalize(values, gain, bias):
    average = jnp.mean(values, axis=-1, keepdims=True)
    centered = values - average
    spread = jnp.mean(centered * centered, axis=-1, keepdims=True)
    return centered * lax.rsqrt(spread + EPSILON) * gain + bias


def cut_kernel(merge_ref, qkv_ref, out_ref, held_hbm, sems):
    core = lax.axis_index("lon") % 2
    for side in range(2):

        @pl.when(core == side)
        def _():
            cuts = [(merge_ref, side * 384, 0, 96), (out_ref, side * 384, 240, 48)]
            cuts += [(qkv_ref, side * 1152 + n * 384, 96 + n * 48, 48) for n in range(3)]
            copies = []
            for member in range(4):
                for n, (source, column, row, rows) in enumerate(cuts):
                    copies.append(
                        pltpu.make_async_copy(
                            source.at[:, pl.ds(column, 384)],
                            held_hbm.at[member, pl.ds(row, rows), :],
                            sems.at[member * 5 + n],
                        )
                    )
            for copy in copies:
                copy.start()
            for copy in copies:
                copy.wait()


def cut(weights):
    return pl.pallas_call(
        cut_kernel,
        out_shape=jax.ShapeDtypeStruct((4, 288, 384), BF16),
        in_specs=[pl.BlockSpec(memory_space=pltpu.VMEM)] * 3,
        out_specs=pl.BlockSpec(memory_space=pl.ANY),
        scratch_shapes=[pltpu.SemaphoreType.DMA((20,))],
        name="cut",
        cost_estimate=pl.CostEstimate(flops=1_000_000, bytes_accessed=1_800_000, transcendentals=0),
    )(*weights)


def left_kernel(fine_ref, left_ref):
    row = lax.broadcasted_iota(jnp.int32, (144, 1), 0)
    source = lax.broadcasted_iota(jnp.int32, (144, 288), 1)
    pick = jnp.where(source == row // 12 * 24 + row % 12, 1.0, 0.0).astype(BF16)
    for level in range(4):
        part = dot(pick, fine_ref[level * 288 : level * 288 + 288])
        left_ref[level * 144 : level * 144 + 144] = part.astype(BF16)


def left_half(fine):
    return pl.pallas_call(
        left_kernel,
        out_shape=jax.ShapeDtypeStruct((576, 384), BF16),
        name="left",
        cost_estimate=pl.CostEstimate(
            flops=200_000_000, bytes_accessed=1_400_000, transcendentals=0
        ),
    )(fine)


def patch_kernel(
    fine_hbm, left_hbm, gain_hbm, bias_hbm, near_ref, far_ref, fine_ref, left_ref, gain_ref, bias_ref, sems
):
    core = lax.axis_index("lon") % 2
    loads = [
        pltpu.make_async_copy(source, target, sems.at[n])
        for n, (source, target) in enumerate(
            ((fine_hbm, fine_ref), (left_hbm, left_ref), (gain_hbm, gain_ref), (bias_hbm, bias_ref))
        )
    ]
    for load in loads:
        load.start()
    row = lax.broadcasted_iota(jnp.int32, (72, 1), 0)
    level, a, b = row // 18, row % 18 // 6, row % 6
    own_at = level * 144 + a * 48 + (6 + b) * 2
    next_at = level * 144 + a * 24 + b * 2
    source = lax.broadcasted_iota(jnp.int32, (72, 576), 1)

    def picks(base, places):
        return [jnp.where(source == base + at, 1.0, 0.0).astype(BF16) for at in places]

    own_picks = picks(own_at, (0, 1, 24, 25))
    for load in loads:
        load.wait()
    for half, ref in ((1 - core, near_ref), (core, far_ref)):
        own = jnp.concatenate(
            [
                fine_ref[pl.ds(pl.multiple_of(level * 288 + half * 144, 144), 144), :]
                for level in range(4)
            ],
            axis=0,
        )
        next_picks = picks(next_at + half * 72, (0, 1, 12, 13))
        for first, fine, chosen in ((0, own, own_picks), (72, left_ref[...], next_picks)):
            parts = [dot(pick, fine) for pick in chosen]
            total = parts[0] + parts[1] + parts[2] + parts[3]
            average = jnp.sum(total, axis=-1, keepdims=True) / 1536
            parts = [part - average for part in parts]
            squares = sum(part * part for part in parts)
            scale = lax.rsqrt(jnp.sum(squares, axis=-1, keepdims=True) / 1536 + EPSILON)
            for k in range(4):
                cols = slice(k * 384, (k + 1) * 384)
                gain, bias = gain_ref[cols].reshape(1, 384), bias_ref[cols].reshape(1, 384)
                ref[first : first + 72, cols] = (parts[k] * scale * gain + bias).astype(BF16)


def patches(fine, left, gain, bias):
    pack = jax.ShapeDtypeStruct((144, 1536), BF16)
    operands = (fine, left, gain, bias)
    return pl.pallas_call(
        patch_kernel,
        out_shape=(pack, pack),
        in_specs=[pl.BlockSpec(memory_space=pltpu.HBM)] * 4,
        out_specs=(pl.BlockSpec(memory_space=pltpu.VMEM),) * 2,
        scratch_shapes=[pltpu.VMEM(value.shape, value.dtype) for value in operands]
        + [pltpu.SemaphoreType.DMA((4,))],
        name="patches",
        compiler_params=pltpu.CompilerParams(vmem_limit_bytes=12 * 1024 * 1024),
        cost_estimate=pl.CostEstimate(
            flops=1_000_000_000, bytes_accessed=1_800_000, transcendentals=0
        ),
    )(*operands)


def frame_order(incoming):
    window = lax.broadcasted_iota(jnp.int32, (288, 1) if incoming else (1, 288), 0 if incoming else 1)
    source = lax.broadcasted_iota(jnp.int32, (288, 288), 1 if incoming else 0)
    pair, rest = window // 144, window % 144
    quad, rest = rest // 36, rest % 36
    level = (2 * pair + rest // 18 + 1) % 4
    place = level * 18 + rest % 18 if incoming else rest % 18 * 4 + level
    return jnp.where(source == quad * 72 + place, 1.0, 0.0).astype(BF16)


def main_kernel(
    p0, p1, a0, a1, a2, a3, b0, b1, b2, b3, gain_ref, bias_ref,
    o0, o1, o2, o3,
    patch_s, merge_s, qkv_s, out_s, proj_s, ctx_s, sems,
):
    core, lat = lax.axis_index("lon") % 2, lax.axis_index("lat")
    x, y = lat % 4, lat // 4
    for source, at in ((p0, 0), (p1, 144)):
        target = patch_s.at[pl.ds(at, 144), :]
        pltpu.make_async_copy(source, target, sems.at[0]).start()

    def scatter(kind, source, k, side):
        def part(base, rows, target, sem, first, width):
            spot = (y + STEPS[k] + 4) % 4 if side == 0 else (x + STEPS[k] + 4) % 4
            cols = pl.ds(side * width + first, 384)
            held = source.at[:, pl.ds(base, rows), :]
            place = target.at[spot, :, :, cols] if side == 0 else target.at[:, spot, :, cols]
            pltpu.make_async_copy(held, place, sems.at[sem]).start()

        if kind == 0:
            part(0, 96, merge_s, 1, 0, 384)
        elif kind == 1:
            for n in range(3):
                part(96 + n * 48, 48, qkv_s, 2, n * 384, 1152)
        else:
            part(240, 48, out_s, 3, 0, 384)

    own, other = (a0, a1, a2, a3), (b0, b1, b2, b3)
    for near_core in range(2):

        @pl.when(core == near_core)
        def _():
            for kind in range(3):
                for blocks, side in ((own, near_core), (other, 1 - near_core)):
                    for k in range(4):
                        scatter(kind, blocks[k], k, side)

    to_window = frame_order(True)
    pltpu.make_async_copy(patch_s, patch_s, sems.at[0]).wait()
    pltpu.make_async_copy(merge_s, merge_s, sems.at[1]).wait()
    coarse = dot(patch_s[...], merge_s[...].reshape(1536, 768)).astype(BF16)
    coarse = dot(to_window, coarse).astype(BF16)
    gain, bias = gain_ref[...].reshape(1, 768), bias_ref[...].reshape(1, 768)
    normed = normalize(coarse.astype(F32), gain, bias).astype(BF16)
    pltpu.make_async_copy(qkv_s, qkv_s, sems.at[2]).wait()
    for n in range(6):
        cols = slice(n * 384, (n + 1) * 384)
        proj_s[:, cols] = dot(normed, qkv_s[:, :, :, cols].reshape(768, 384)).astype(BF16)

    lane = lax.broadcasted_iota(jnp.int32, (1, 128), 1) // 32
    query = lax.broadcasted_iota(jnp.int32, (576, 1), 0) % 144
    key = lax.broadcasted_iota(jnp.int32, (1, 144), 1)
    wraps = lat == jnp.where(core == 0, 15, 0)
    row_apart = ((query // 72) != (key // 72)) & wraps
    level_apart = (query // 18 % 2) != (key // 18 % 2)
    low = F32(-1e30)
    for pair in range(2):
        rows = slice(pair * 144, (pair + 1) * 144)
        apart = (row_apart | level_apart) if pair == 1 else row_apart
        penalty = jnp.where(apart, low, 0.0)
        for g in range(6):
            q = proj_s[rows, g * 128 : (g + 1) * 128]
            k = proj_s[rows, 768 + g * 128 : 768 + (g + 1) * 128]
            v = proj_s[rows, 1536 + g * 128 : 1536 + (g + 1) * 128]
            stacked = jnp.concatenate(
                [jnp.where(lane == h, q, jnp.zeros_like(q)) for h in range(4)], axis=0
            )
            scores = lax.dot_general(
                stacked, k, (((1,), (1,)), ((), ())), preferred_element_type=F32
            )
            scores = scores * (32**-0.5) + penalty
            peak = jnp.max(scores, axis=-1, keepdims=True)
            weights = jnp.exp(scores - peak)
            total = jnp.sum(weights, axis=-1, keepdims=True)
            mixed = dot(weights.astype(BF16), v) / total
            picked = mixed[:144] * jnp.where(lane == 0, 1.0, 0.0)
            for h in range(1, 4):
                picked = jnp.where(lane == h, mixed[h * 144 : (h + 1) * 144], picked)
            ctx_s[rows, g * 128 : (g + 1) * 128] = picked.astype(BF16)

    pltpu.make_async_copy(out_s, out_s, sems.at[3]).wait()
    branch = dot(ctx_s[...], out_s[...].reshape(768, 768))
    result = (coarse.astype(F32) + branch).astype(BF16)
    result = dot(frame_order(False), result).astype(BF16)
    for ref, first, count in ((o0, 0, 18), (o1, 72, 18), (o2, 144, 18), (o3, 216, 18)):
        for place in range(count):
            at = first + place * 4
            ref[place] = result[at : at + 4]


def main(quads, own, other, gain, bias):
    any_space = pl.BlockSpec(memory_space=pl.ANY)
    vmem = pl.BlockSpec(memory_space=pltpu.VMEM)
    quad = jax.ShapeDtypeStruct((18, 4, 768), BF16)
    return pl.pallas_call(
        main_kernel,
        out_shape=(quad,) * 4,
        in_specs=[any_space] * 10 + [vmem] * 2,
        out_specs=(vmem,) * 4,
        scratch_shapes=[
            pltpu.VMEM((288, 1536), BF16),
            pltpu.VMEM((4, 4, 96, 768), BF16),
            pltpu.VMEM((4, 4, 48, 2304), BF16),
            pltpu.VMEM((4, 4, 48, 768), BF16),
            pltpu.VMEM((288, 2304), BF16),
            pltpu.VMEM((288, 768), BF16),
            pltpu.SemaphoreType.DMA((4,)),
        ],
        name="main",
        compiler_params=pltpu.CompilerParams(vmem_limit_bytes=20 * 1024 * 1024),
        cost_estimate=pl.CostEstimate(
            flops=5_000_000_000, bytes_accessed=9_000_000, transcendentals=2_000_000
        ),
    )(*quads, *own, *other, gain, bias)


def tiles(quad):
    return quad.reshape(3, 6, 4, 768)


def shards(
    fine_input,
    merge_gain,
    merge_bias,
    merge_weight,
    coarse_gain,
    coarse_bias,
    coarse_qkv,
    coarse_out,
):
    weights = (merge_weight, coarse_qkv, coarse_out)
    fine = fine_input.reshape(1152, 384)
    block = lax.all_to_all(cut(weights), AXES, 0, 0, axis_index_groups=near_groups())
    left = left_half(fine)
    left = moved(left, shift_pairs(-1, 0))
    own = [block] + [moved(block, far_pairs(step)) for step in (1, -1, 2)]
    near_rows, far_rows = patches(fine, left, merge_gain, merge_bias)
    far_rows = moved(far_rows, shift_pairs(0, -1))
    other = []
    for piece in own:
        other.append(moved(piece, swap_pairs()))
    result = main([near_rows, far_rows], own, other, coarse_gain, coarse_bias)
    near_left = moved(result[3], shift_pairs(-1, 1, back=True))
    far_right = moved(result[2], shift_pairs(0, -1, back=True))
    far_left = moved(result[1], shift_pairs(-1, 0, back=True))
    near = [tiles(near_left), tiles(result[0])]
    far = [tiles(far_left), tiles(far_right)]
    upper = lax.axis_index("lon") % 2 == 1
    above = jnp.concatenate([jnp.where(upper, a, b) for a, b in zip(near, far)], axis=1)
    below = jnp.concatenate([jnp.where(upper, b, a) for a, b in zip(near, far)], axis=1)
    return jnp.concatenate([above, below], axis=0).transpose(2, 0, 1, 3)


def solution(mesh):
    placed = (
        P(None, "lat", "lon", None),
        P(),
        P(),
        P("lat", None),
        P(),
        P(),
        P("lat", None),
        P("lat", None),
    )
    return jax.shard_map(
        shards, mesh=mesh, in_specs=placed, out_specs=P(None, "lat", "lon", None), check_vma=False
    )
```

```python
import jax
import jax.numpy as jnp
from jax import lax
from jax.experimental import pallas as pl
from jax.experimental.pallas import tpu as pltpu
from jax.sharding import PartitionSpec as P


EPSILON = 1e-05
AXES = ("lon", "lat")
F32 = jnp.float32
BF16 = jnp.bfloat16

DEVICES = 512


def coords_of(flat):
    lat, lon = flat % 16, flat // 16
    return lat % 4, (lon // 16) * 4 + lat // 4, lon // 2 % 8, lon % 2


def flat_of(x, y, z, core):
    x, y, z = x % 4, y % 8, z % 8
    return (((y // 4) * 8 + z) * 2 + core) * 16 + (y % 4) * 4 + x


def ring_step(dx, dy, x, y):
    if dy == 2:
        dy = 2 if y % 2 == 0 else -2
    return x + dx, y + dy


def far_pairs(step):
    pairs = []
    for flat in range(DEVICES):
        x, y, z, core = coords_of(flat)
        nx, ny = ring_step(step if core == 1 else 0, step if core == 0 else 0, x, y)
        pairs.append((flat, flat_of(nx, ny, z, core)))
    return pairs


def near_groups():
    groups = {}
    for flat in range(DEVICES):
        x, y, z, core = coords_of(flat)
        key = (core, y, z) if core == 0 else (core, x, z, y // 4)
        groups.setdefault(key, []).append((x if core == 0 else y, flat))
    return [[flat for _, flat in sorted(group)] for group in groups.values()]


def swap_pairs():
    pairs = []
    for flat in range(DEVICES):
        x, y, z, core = coords_of(flat)
        pairs.append((flat, flat_of(x, y, z, 1 - core)))
    return pairs


def shift_pairs(dlon, dlat, back=False):
    pairs = []
    for flat in range(DEVICES):
        lon, lat = flat // 16, flat % 16
        sign = 1 if lon % 2 == 0 else -1
        target = (lon + dlon) % 32 * 16 + (lat + sign * dlat) % 16
        pairs.append((target, flat) if back else (flat, target))
    return pairs


def moved(value, pairs):
    return lax.ppermute(value, AXES, pairs)


STEPS = (0, -1, 1, 2)


def dot(a, b):
    return jnp.dot(a, b, preferred_element_type=F32)


def normalize(values, gain, bias):
    average = jnp.mean(values, axis=-1, keepdims=True)
    centered = values - average
    spread = jnp.mean(centered * centered, axis=-1, keepdims=True)
    return centered * lax.rsqrt(spread + EPSILON) * gain + bias


def cut_kernel(fine_ref, merge_ref, qkv_ref, out_ref, left_ref, held_hbm, sems):
    core = lax.axis_index("lon") % 2
    for side in range(2):

        @pl.when(core == side)
        def _():
            cuts = [(merge_ref, side * 384, 0, 96), (out_ref, side * 384, 240, 48)]
            cuts += [(qkv_ref, side * 1152 + n * 384, 96 + n * 48, 48) for n in range(3)]
            copies = []
            for member in range(4):
                for n, (source, column, row, rows) in enumerate(cuts):
                    copies.append(
                        pltpu.make_async_copy(
                            source.at[:, pl.ds(column, 384)],
                            held_hbm.at[member, pl.ds(row, rows), :],
                            sems.at[member * 5 + n],
                        )
                    )
            for copy in copies:
                copy.start()
            row = lax.broadcasted_iota(jnp.int32, (144, 1), 0)
            source = lax.broadcasted_iota(jnp.int32, (144, 288), 1)
            pick = jnp.where(source == row // 12 * 24 + row % 12, 1.0, 0.0).astype(BF16)
            for level in range(4):
                part = dot(pick, fine_ref[level * 288 : level * 288 + 288])
                left_ref[level * 144 : level * 144 + 144] = part.astype(BF16)
            for copy in copies:
                copy.wait()


def cut(fine, weights):
    vmem = pl.BlockSpec(memory_space=pltpu.VMEM)
    return pl.pallas_call(
        cut_kernel,
        out_shape=(
            jax.ShapeDtypeStruct((576, 384), BF16),
            jax.ShapeDtypeStruct((4, 288, 384), BF16),
        ),
        in_specs=[vmem] * 4,
        out_specs=(vmem, pl.BlockSpec(memory_space=pl.ANY)),
        scratch_shapes=[pltpu.SemaphoreType.DMA((20,))],
        name="cut",
        cost_estimate=pl.CostEstimate(
            flops=200_000_000, bytes_accessed=3_000_000, transcendentals=0
        ),
    )(fine, *weights)


def patch_kernel(
    fine_hbm, left_hbm, gain_hbm, bias_hbm, near_ref, far_ref, fine_ref, left_ref, gain_ref, bias_ref, sems
):
    core = lax.axis_index("lon") % 2
    loads = [
        pltpu.make_async_copy(source, target, sems.at[n])
        for n, (source, target) in enumerate(
            ((fine_hbm, fine_ref), (left_hbm, left_ref), (gain_hbm, gain_ref), (bias_hbm, bias_ref))
        )
    ]
    for load in loads:
        load.start()
    row = lax.broadcasted_iota(jnp.int32, (72, 1), 0)
    level, a, b = row // 18, row % 18 // 6, row % 6
    own_at = level * 144 + a * 48 + (6 + b) * 2
    next_at = level * 144 + a * 24 + b * 2
    source = lax.broadcasted_iota(jnp.int32, (72, 576), 1)

    def picks(base, places):
        return [jnp.where(source == base + at, 1.0, 0.0).astype(BF16) for at in places]

    own_picks = picks(own_at, (0, 1, 24, 25))
    for load in loads:
        load.wait()
    for half, ref in ((1 - core, near_ref), (core, far_ref)):
        own = jnp.concatenate(
            [
                fine_ref[pl.ds(pl.multiple_of(level * 288 + half * 144, 144), 144), :]
                for level in range(4)
            ],
            axis=0,
        )
        next_picks = picks(next_at + half * 72, (0, 1, 12, 13))
        for first, fine, chosen in ((0, own, own_picks), (72, left_ref[...], next_picks)):
            parts = [dot(pick, fine) for pick in chosen]
            total = parts[0] + parts[1] + parts[2] + parts[3]
            average = jnp.sum(total, axis=-1, keepdims=True) / 1536
            parts = [part - average for part in parts]
            squares = sum(part * part for part in parts)
            scale = lax.rsqrt(jnp.sum(squares, axis=-1, keepdims=True) / 1536 + EPSILON)
            for k in range(4):
                cols = slice(k * 384, (k + 1) * 384)
                gain, bias = gain_ref[cols].reshape(1, 384), bias_ref[cols].reshape(1, 384)
                ref[first : first + 72, cols] = (parts[k] * scale * gain + bias).astype(BF16)


def patches(fine, left, gain, bias):
    pack = jax.ShapeDtypeStruct((144, 1536), BF16)
    operands = (fine, left, gain, bias)
    return pl.pallas_call(
        patch_kernel,
        out_shape=(pack, pack),
        in_specs=[pl.BlockSpec(memory_space=pltpu.HBM)] * 4,
        out_specs=(pl.BlockSpec(memory_space=pltpu.VMEM),) * 2,
        scratch_shapes=[pltpu.VMEM(value.shape, value.dtype) for value in operands]
        + [pltpu.SemaphoreType.DMA((4,))],
        name="patches",
        compiler_params=pltpu.CompilerParams(vmem_limit_bytes=12 * 1024 * 1024),
        cost_estimate=pl.CostEstimate(
            flops=1_000_000_000, bytes_accessed=1_800_000, transcendentals=0
        ),
    )(*operands)


def frame_order(incoming):
    window = lax.broadcasted_iota(jnp.int32, (288, 1) if incoming else (1, 288), 0 if incoming else 1)
    source = lax.broadcasted_iota(jnp.int32, (288, 288), 1 if incoming else 0)
    pair, rest = window // 144, window % 144
    quad, rest = rest // 36, rest % 36
    level = (2 * pair + rest // 18 + 1) % 4
    place = level * 18 + rest % 18 if incoming else rest % 18 * 4 + level
    return jnp.where(source == quad * 72 + place, 1.0, 0.0).astype(BF16)


def main_kernel(
    p0, p1, a0, a1, a2, a3, b0, b1, b2, b3, gain_ref, bias_ref,
    o0, o1, o2, o3,
    patch_s, merge_s, qkv_s, out_s, proj_s, ctx_s, sems,
):
    core, lat = lax.axis_index("lon") % 2, lax.axis_index("lat")
    x, y = lat % 4, lat // 4
    for source, at in ((p0, 0), (p1, 144)):
        target = patch_s.at[pl.ds(at, 144), :]
        pltpu.make_async_copy(source, target, sems.at[0]).start()

    def scatter(kind, source, k, side):
        def part(base, rows, target, sem, first, width):
            spot = (y + STEPS[k] + 4) % 4 if side == 0 else (x + STEPS[k] + 4) % 4
            cols = pl.ds(side * width + first, 384)
            held = source.at[:, pl.ds(base, rows), :]
            place = target.at[spot, :, :, cols] if side == 0 else target.at[:, spot, :, cols]
            pltpu.make_async_copy(held, place, sems.at[sem]).start()

        if kind == 0:
            part(0, 96, merge_s, 1, 0, 384)
        elif kind == 1:
            for n in range(3):
                part(96 + n * 48, 48, qkv_s, 2, n * 384, 1152)
        else:
            part(240, 48, out_s, 3, 0, 384)

    own, other = (a0, a1, a2, a3), (b0, b1, b2, b3)
    for near_core in range(2):

        @pl.when(core == near_core)
        def _():
            for kind in range(3):
                for blocks, side in ((own, near_core), (other, 1 - near_core)):
                    for k in range(4):
                        scatter(kind, blocks[k], k, side)

    to_window = frame_order(True)
    pltpu.make_async_copy(patch_s, patch_s, sems.at[0]).wait()
    pltpu.make_async_copy(merge_s, merge_s, sems.at[1]).wait()
    coarse = dot(patch_s[...], merge_s[...].reshape(1536, 768)).astype(BF16)
    coarse = dot(to_window, coarse).astype(BF16)
    gain, bias = gain_ref[...].reshape(1, 768), bias_ref[...].reshape(1, 768)
    normed = normalize(coarse.astype(F32), gain, bias).astype(BF16)
    pltpu.make_async_copy(qkv_s, qkv_s, sems.at[2]).wait()
    for n in range(6):
        cols = slice(n * 384, (n + 1) * 384)
        proj_s[:, cols] = dot(normed, qkv_s[:, :, :, cols].reshape(768, 384)).astype(BF16)

    lane = lax.broadcasted_iota(jnp.int32, (1, 128), 1) // 32
    query = lax.broadcasted_iota(jnp.int32, (576, 1), 0) % 144
    key = lax.broadcasted_iota(jnp.int32, (1, 144), 1)
    wraps = lat == jnp.where(core == 0, 15, 0)
    row_apart = ((query // 72) != (key // 72)) & wraps
    level_apart = (query // 18 % 2) != (key // 18 % 2)
    low = F32(-1e30)
    for pair in range(2):
        rows = slice(pair * 144, (pair + 1) * 144)
        apart = (row_apart | level_apart) if pair == 1 else row_apart
        penalty = jnp.where(apart, low, 0.0)
        for g in range(6):
            q = proj_s[rows, g * 128 : (g + 1) * 128]
            k = proj_s[rows, 768 + g * 128 : 768 + (g + 1) * 128]
            v = proj_s[rows, 1536 + g * 128 : 1536 + (g + 1) * 128]
            stacked = jnp.concatenate(
                [jnp.where(lane == h, q, jnp.zeros_like(q)) for h in range(4)], axis=0
            )
            scores = lax.dot_general(
                stacked, k, (((1,), (1,)), ((), ())), preferred_element_type=F32
            )
            scores = scores * (32**-0.5) + penalty
            peak = jnp.max(scores, axis=-1, keepdims=True)
            weights = jnp.exp(scores - peak)
            total = jnp.sum(weights, axis=-1, keepdims=True)
            mixed = dot(weights.astype(BF16), v) / total
            picked = mixed[:144] * jnp.where(lane == 0, 1.0, 0.0)
            for h in range(1, 4):
                picked = jnp.where(lane == h, mixed[h * 144 : (h + 1) * 144], picked)
            ctx_s[rows, g * 128 : (g + 1) * 128] = picked.astype(BF16)

    pltpu.make_async_copy(out_s, out_s, sems.at[3]).wait()
    branch = dot(ctx_s[...], out_s[...].reshape(768, 768))
    result = (coarse.astype(F32) + branch).astype(BF16)
    result = dot(frame_order(False), result).astype(BF16)
    for ref, first, count in ((o0, 0, 18), (o1, 72, 18), (o2, 144, 18), (o3, 216, 18)):
        for place in range(count):
            at = first + place * 4
            ref[place] = result[at : at + 4]


def main(quads, own, other, gain, bias):
    any_space = pl.BlockSpec(memory_space=pl.ANY)
    vmem = pl.BlockSpec(memory_space=pltpu.VMEM)
    quad = jax.ShapeDtypeStruct((18, 4, 768), BF16)
    return pl.pallas_call(
        main_kernel,
        out_shape=(quad,) * 4,
        in_specs=[any_space] * 10 + [vmem] * 2,
        out_specs=(vmem,) * 4,
        scratch_shapes=[
            pltpu.VMEM((288, 1536), BF16),
            pltpu.VMEM((4, 4, 96, 768), BF16),
            pltpu.VMEM((4, 4, 48, 2304), BF16),
            pltpu.VMEM((4, 4, 48, 768), BF16),
            pltpu.VMEM((288, 2304), BF16),
            pltpu.VMEM((288, 768), BF16),
            pltpu.SemaphoreType.DMA((4,)),
        ],
        name="main",
        compiler_params=pltpu.CompilerParams(vmem_limit_bytes=20 * 1024 * 1024),
        cost_estimate=pl.CostEstimate(
            flops=5_000_000_000, bytes_accessed=9_000_000, transcendentals=2_000_000
        ),
    )(*quads, *own, *other, gain, bias)


def tiles(quad):
    return quad.reshape(3, 6, 4, 768)


def shards(
    fine_input,
    merge_gain,
    merge_bias,
    merge_weight,
    coarse_gain,
    coarse_bias,
    coarse_qkv,
    coarse_out,
):
    weights = (merge_weight, coarse_qkv, coarse_out)
    fine = fine_input.reshape(1152, 384)
    left, held = cut(fine, weights)
    block = lax.all_to_all(held, AXES, 0, 0, axis_index_groups=near_groups())
    left = moved(left, shift_pairs(-1, 0))
    own = [block] + [moved(block, far_pairs(step)) for step in (1, -1, 2)]
    near_rows, far_rows = patches(fine, left, merge_gain, merge_bias)
    far_rows = moved(far_rows, shift_pairs(0, -1))
    other = []
    for piece in own:
        other.append(moved(piece, swap_pairs()))
    result = main([near_rows, far_rows], own, other, coarse_gain, coarse_bias)
    near_left = moved(result[3], shift_pairs(-1, 1, back=True))
    far_right = moved(result[2], shift_pairs(0, -1, back=True))
    far_left = moved(result[1], shift_pairs(-1, 0, back=True))
    near = [tiles(near_left), tiles(result[0])]
    far = [tiles(far_left), tiles(far_right)]
    upper = lax.axis_index("lon") % 2 == 1
    above = jnp.concatenate([jnp.where(upper, a, b) for a, b in zip(near, far)], axis=1)
    below = jnp.concatenate([jnp.where(upper, b, a) for a, b in zip(near, far)], axis=1)
    return jnp.concatenate([above, below], axis=0).transpose(2, 0, 1, 3)


def solution(mesh):
    placed = (
        P(None, "lat", "lon", None),
        P(),
        P(),
        P("lat", None),
        P(),
        P(),
        P("lat", None),
        P("lat", None),
    )
    return jax.shard_map(
        shards, mesh=mesh, in_specs=placed, out_specs=P(None, "lat", "lon", None), check_vma=False
    )
```
